32 devices in a mesh: dp: 8 (over z, y), mp: 4 (over x, core).
Axes of the slice: x: 2, y: 2, z: 4, core: 2. Of those that a mesh axis runs over, the one named last changes fastest.
Arguments:
- gradient: bfloat16 [1, 4096, 4096], P(None, 'mp', 'dp'), may hold values from -6 to 6
- first_moment: float32 [1, 4096, 4096], P(None, 'mp', 'dp'), may hold values from -3 to 3
- second_moment: float32 [1, 4096, 4096], P(None, 'mp', 'dp'), may hold values from 0.0625 to 1
- left_factor: float32 [1, 4096, 4096], P(None, 'mp', 'dp'), may hold values from -18 to 18
- right_factor: float32 [1, 4096, 4096], P(None, 'mp', 'dp'), may hold values from -18 to 18
- left_basis: bfloat16 [1, 4096, 4096], P(None, 'dp', 'mp'), may hold values from -0.09375 to 0.09375
- right_basis: bfloat16 [1, 4096, 4096], P(None, 'mp', 'dp'), may hold values from -0.09375 to 0.09375
Outputs:
- new_first_moment: float32 [1, 4096, 4096], P(None, 'mp', 'dp')
- new_second_moment: float32 [1, 4096, 4096], P(None, 'mp', 'dp')
- new_left_factor: float32 [1, 4096, 4096], P(None, 'mp', 'dp')
- new_right_factor: float32 [1, 4096, 4096], P(None, 'mp', 'dp')
- update: bfloat16 [1, 4096, 4096], P(None, 'mp', 'dp')
The draws below stay inside these ranges and needn't reach their ends.
All inputs are finite; a program needn't handle non-finite values.
Results may differ from the reference program's by a relative error of at most 0.014.
Values may be sent and summed in bfloat16 or wider, within the bound.
A program may use at most 128 MiB of HBM per device.

```python
import math
import jax
import jax.numpy as jnp
from jax import lax

B = 4096
BLOCKS = 1


def shard_levels(rng, dims, split, low, high):
    def one(position, shards_of):
        steps = jax.random.uniform(jax.random.fold_in(jax.random.fold_in(rng, 6), position), (shards_of,), jnp.float32, low / len(split), high / len(split))
        return jnp.repeat(jnp.exp(steps), dims[position] // shards_of).reshape((-1,) + (1,) * (len(dims) - position - 1))

    level = one(*split[0])
    for cut in split[1:]:
        level = level * one(*cut)
    return level


def scatter_about(stream_key, shape, spread, reach, split=(), dtype=jnp.bfloat16):
    drawn = spread * jax.random.normal(stream_key, shape, jnp.float32)
    if split:
        drawn = drawn * shard_levels(stream_key, shape, split, -0.22, 0.18)
    return jnp.clip(drawn, -reach, reach).astype(dtype)


def setup_inputs(seed: int = 0) -> dict:
    splits = jax.random.split(jax.random.key(seed), 8)
    gradient = scatter_about(splits[0], (BLOCKS, B, B), 1.0, 6.0, ((1, 4), (2, 8)))
    first_moment = scatter_about(splits[1], (BLOCKS, B, B), 0.5, 3.0, ((1, 4), (2, 8)), jnp.float32)
    second_moment = jnp.clip(jnp.exp(math.log(1.0) - 2.7725887 * jax.random.uniform(splits[2], (BLOCKS, B, B), jnp.float32) ** shard_levels(splits[2], (BLOCKS, B, B), ((1, 4), (2, 8)), -0.2, 0.2)), 0.0625, 1.0)
    left_factor = scatter_about(splits[3], (BLOCKS, B, B), 3.0, 18.0, ((1, 4), (2, 8)), jnp.float32)
    right_factor = scatter_about(splits[4], (BLOCKS, B, B), 3.0, 18.0, ((1, 4), (2, 8)), jnp.float32)
    left_basis = scatter_about(splits[5], (BLOCKS, B, B), B ** -0.5, 0.09375, ((1, 8), (2, 4)))
    right_basis = scatter_about(splits[6], (BLOCKS, B, B), B ** -0.5, 0.09375, ((1, 4), (2, 8)))
    return {"gradient": gradient, "first_moment": first_moment, "second_moment": second_moment, "left_factor": left_factor, "right_factor": right_factor, "left_basis": left_basis, "right_basis": right_basis}


decay_moment = 0.95
decay_factor = 0.95
epsilon = 1e-08

def product(left, right):
    return jnp.dot(left.astype(jnp.float32), right.astype(jnp.float32), precision=lax.Precision.HIGHEST)

def single_block(operands):
    gradient, first_moment, second_moment, left_factor, right_factor, left_basis, right_basis = operands
    scale = 1.0 - decay_factor
    new_left = decay_factor * left_factor + scale * product(gradient, gradient.T)
    new_right = decay_factor * right_factor + scale * product(gradient.T, gradient)
    rotated_left = product(left_basis.T, gradient).astype(jnp.bfloat16)
    rotated = product(rotated_left, right_basis)
    new_first = decay_moment * first_moment + (1.0 - decay_moment) * rotated
    new_second = decay_moment * second_moment + (1.0 - decay_moment) * rotated * rotated
    direction = (new_first / (jnp.sqrt(new_second) + epsilon)).astype(jnp.bfloat16)
    back_left = product(left_basis, direction).astype(jnp.bfloat16)
    update = product(back_left, right_basis.T).astype(jnp.bfloat16)
    return (new_first, new_second, new_left, new_right, update)

def reference(gradient, first_moment, second_moment, left_factor, right_factor, left_basis, right_basis):
    first_out, second_out, left_out, right_out, update_out = lax.map(single_block, (gradient, first_moment, second_moment, left_factor, right_factor, left_basis, right_basis))
    return (first_out, second_out, left_out, right_out, update_out)
```

```python
import jax
import jax.numpy as jnp
from jax import lax
from jax.sharding import PartitionSpec as P

decay_moment = 0.95
decay_factor = 0.95
epsilon = 1e-08
bf16, f32 = jnp.bfloat16, jnp.float32
update_chunks = 2


def bits_of(count):
    return [1 << i for i in range(count.bit_length() - 1)]


def swap(value, count, bit):
    return lax.ppermute(value, "mp", [(i, i ^ bit) for i in range(count)])


def gather_rows(block, count):
    pieces = {0: block}
    for bit in reversed(bits_of(count)):
        for j in list(pieces):
            pieces[j ^ bit] = swap(pieces[j], count, bit)
    me, rows = lax.axis_index("mp"), block.shape[1]
    whole = jnp.zeros((block.shape[0], rows * count, block.shape[2]), block.dtype)
    for j, piece in pieces.items():
        whole = lax.dynamic_update_slice_in_dim(whole, piece, (me ^ j) * rows, 1)
    return whole


def scatter_rows(term, count):
    me, rows = lax.axis_index("mp"), term.shape[1] // count
    held = {
        j: lax.dynamic_slice_in_dim(term, (me ^ j) * rows, rows, 1) for j in range(count)
    }
    for bit in bits_of(count):
        for j in [j for j in held if j & bit]:
            arrived = swap(held.pop(j).astype(bf16), count, bit)
            held[j ^ bit] = held[j ^ bit] + arrived.astype(f32)
    return held[0]


def paired_rows(row_grad, dp, mp):
    depth, rows = row_grad.shape[2] // dp, row_grad.shape[1]
    d, m = lax.axis_index("dp"), lax.axis_index("mp")
    here = lax.dynamic_slice_in_dim(row_grad, lax.rem(d * depth, rows), depth, 1)
    owner = (d * depth) // rows
    held_bits = 0
    for bit in reversed(bits_of(mp)):
        pairs = []
        for i in range(dp):
            first = i * depth // rows
            for k in range(mp):
                if (k ^ first) & ~held_bits == 0:
                    pairs.append((i * mp + k, i * mp + (k ^ bit)))
        arrived = lax.ppermute(here, ("dp", "mp"), pairs)
        here = jnp.where(((m ^ owner) & bit) == 0, here, arrived)
        held_bits |= bit
    return here


def solution(mesh):
    dp, mp = mesh.shape["dp"], mesh.shape["mp"]

    def per_device(
        gradient, first_moment, second_moment, left_factor, right_factor, left_basis, right_basis
    ):
        scale = 1.0 - decay_factor
        row_grad = lax.all_gather(gradient, "dp", axis=2, tiled=True)
        column_left = lax.all_gather(left_basis, "dp", axis=1, tiled=True)
        column_right = gather_rows(right_basis, mp)

        rotated_right = jnp.einsum(
            "brn,bnc->brc", row_grad, column_right, preferred_element_type=f32
        ).astype(bf16)
        column_rotated = gather_rows(rotated_right, mp)
        right_sum = scatter_rows(
            jnp.einsum("bkr,bkc->brc", row_grad, gradient, preferred_element_type=f32), mp
        )
        row_block = paired_rows(row_grad, dp, mp)
        left_sum = jnp.einsum("brk,bck->brc", row_grad, row_block, preferred_element_type=f32)

        rotated = jnp.einsum(
            "bkr,bkc->brc", column_left, column_rotated, preferred_element_type=f32
        )
        new_first = decay_moment * first_moment + (1.0 - decay_moment) * rotated
        new_second = decay_moment * second_moment + (1.0 - decay_moment) * rotated * rotated
        direction = (new_first / (jnp.sqrt(new_second) + epsilon)).astype(bf16)

        blocks, whole, width = column_right.shape
        split = column_right.reshape(blocks, dp, whole // dp, width)
        part = whole // dp // update_chunks
        pieces = []
        for i in range(update_chunks):
            rows = split[:, :, i * part : (i + 1) * part].reshape(blocks, dp * part, width)
            back_term = jnp.einsum(
                "bjc,brc->bjr", rows, direction, preferred_element_type=f32
            ).astype(bf16)
            back = lax.psum_scatter(back_term, "dp", scatter_dimension=1, tiled=True)
            update_term = jnp.einsum(
                "bkr,bjr->bkj", column_left, back, preferred_element_type=f32
            )
            pieces.append(scatter_rows(update_term, mp).astype(bf16))
        update = jnp.concatenate(pieces, axis=2)

        new_left = decay_factor * left_factor + scale * left_sum
        new_right = decay_factor * right_factor + scale * right_sum
        return (new_first, new_second, new_left, new_right, update)

    return jax.shard_map(
        per_device,
        mesh=mesh,
        in_specs=(P(None, "mp", "dp"),) * 5 + (P(None, "dp", "mp"), P(None, "mp", "dp")),
        out_specs=(P(None, "mp", "dp"),) * 5,
        check_vma=False,
    )
```
